256 devices in a mesh: seq: 64 (over z, y, core), head: 4 (over x).
Axes of the slice: x: 4, y: 4, z: 8, core: 2. Of those that a mesh axis runs over, the one named last changes fastest.
Arguments:
- query_rows: bfloat16 [32768, 4096], P('seq', 'head'), may hold values from -6 to 6
- key_rows: bfloat16 [32768, 4096], P('seq', 'head'), may hold values from -2 to 2
- value_rows: bfloat16 [32768, 4096], P('seq', 'head'), may hold values from -6 to 6
- key_gain: float32 [32], P('head'), may hold values from 0.9 to 1.85, as said below
- regularizer: float32 [32], P('head'), may hold values from 0.5 to 4
Outputs:
- readout: bfloat16 [32768, 4096], P('seq', 'head')
The draws below stay inside these ranges and needn't reach their ends.
Inputs may be any that keep to these rules, and one draw needn't show every extreme that they name: `key_gain`: one positive gain for each head.
All inputs are finite; a program needn't handle non-finite values.
Results may differ from the reference program's by a relative error of at most 0.006.
Values sent between devices are 32-bit elements; how exact they have to be, the bound alone decides.
A program may use at most 192 MiB of HBM per device.

```python
import math
import jax
import jax.numpy as jnp
from jax import lax

DH = 128
HEADS = 32
TOK_DEV = 512
NS_STEPS = 8
REFINE = 2
SEQ = 32768


def draw_key_gain(key, part):
    position = jnp.arange(HEADS, dtype=jnp.float32) / (HEADS - 1)
    return jnp.exp(0.5 * position + jax.random.uniform(key, (HEADS,), jnp.float32, -0.1, 0.1))


def draw_key_rows(key, part):
    column_key = jax.random.fold_in(key, 11)
    entry_key = jax.random.fold_in(key, 12)
    width = HEADS * DH
    amplitude = jnp.exp(jax.random.uniform(column_key, (width,), jnp.float32, math.log(0.3), math.log(2.4)))
    entries = jax.random.truncated_normal(entry_key, -4.0, 4.0, (SEQ, width), jnp.float32)
    return (entries * amplitude[None, :] / math.sqrt(DH)).astype(jnp.bfloat16)


def steps_of(key, dims, shards, low, largest):
    level = 1.0
    for axis_at, blocks in shards:
        heights = jax.random.uniform(jax.random.fold_in(jax.random.fold_in(key, 6), axis_at), (blocks,), jnp.float32, low / len(shards), largest / len(shards))
        level = level * jnp.repeat(jnp.exp(heights), dims[axis_at] // blocks).reshape((-1,) + (1,) * (len(dims) - 1 - axis_at))
    return level


def gaussian(stream_key, extent, scale, most, cuts=(), held_as=jnp.bfloat16):
    gain = steps_of(stream_key, extent, cuts, -0.22, 0.18) if cuts else 1.0
    values = jax.random.normal(stream_key, extent, jnp.float32) * scale * gain
    return jnp.minimum(jnp.maximum(values, -most), most).astype(held_as)


def setup_inputs(seed: int = 0) -> dict:
    seeds = jax.random.split(jax.random.key(seed), 6)
    return {
        "query_rows": gaussian(seeds[0], (SEQ, HEADS * DH), 1.0, 6.0, ((0, 64), (1, 4))),
        "key_rows": draw_key_rows(jax.random.fold_in(seeds[5], 71), 0),
        "value_rows": gaussian(seeds[2], (SEQ, HEADS * DH), 1.0, 6.0, ((0, 64), (1, 4))),
        "key_gain": draw_key_gain(jax.random.fold_in(seeds[5], 71), 0),
        "regularizer": jnp.clip(jnp.exp(math.log(4.0) - 2.0794415 * jax.random.uniform(seeds[4], (HEADS,), jnp.float32) ** steps_of(seeds[4], (HEADS,), ((0, 4),), -0.2, 0.2)), 0.5, 4.0),
    }


highest = lax.Precision.HIGHEST

def contract_rows(left, right):
    return lax.dot_general(left, right, (((1,), (1,)), ((), ())), preferred_element_type=jnp.float32)

def invert_scaled(end_matrix, spectral_bound):
    identity = jnp.eye(end_matrix.shape[-1], dtype=jnp.float32)
    approx = identity[None, :, :] / spectral_bound[:, None, None]
    for iteration in range(NS_STEPS):
        product = jnp.einsum('hij,hjk->hik', end_matrix, approx, precision=highest)
        approx = jnp.einsum('hij,hjk->hik', approx, 2.0 * identity - product, precision=highest)
    return approx

def solve_head(operands):
    query_head, key_head, value_head, base_matrix, precond, cross_matrix = operands
    length = query_head.shape[0]
    causal = jnp.arange(length)[:, None] >= jnp.arange(length)[None, :]
    query_float = query_head.astype(jnp.float32)
    solution = jnp.dot(query_float, precond, precision=highest)
    for repeat in range(REFINE):
        scores = jnp.where(causal, contract_rows(solution.astype(jnp.bfloat16), key_head), 0.0).astype(jnp.bfloat16)
        in_block = jnp.dot(scores, key_head, preferred_element_type=jnp.float32)
        residual = query_float - jnp.dot(solution, base_matrix, precision=highest) - in_block
        solution = solution + jnp.dot(residual, precond, precision=highest)
    scores = jnp.where(causal, contract_rows(solution.astype(jnp.bfloat16), key_head), 0.0).astype(jnp.bfloat16)
    total = jnp.dot(solution, cross_matrix, precision=highest) + jnp.dot(scores, value_head, preferred_element_type=jnp.float32)
    return total.astype(jnp.bfloat16)

def reference(query_rows, key_rows, value_rows, key_gain, regularizer):
    block_count = query_rows.shape[0] // TOK_DEV
    split_shape = (block_count, TOK_DEV, HEADS, DH)
    identity = jnp.eye(DH, dtype=jnp.float32)

    def block_step(carry, operands):
        prior_gram, prior_cross = carry
        query_block, key_block, value_block = operands
        scaled = (key_block.astype(jnp.float32) * key_gain[None, :, None]).astype(jnp.bfloat16)
        scaled_float = scaled.astype(jnp.float32)
        gram_block = jnp.einsum('thd,the->hde', scaled_float, scaled_float, precision=highest)
        cross_block = jnp.einsum('thd,the->hde', scaled_float, value_block.astype(jnp.float32), precision=highest)
        base_matrix = regularizer[:, None, None] * identity + prior_gram
        end_matrix = base_matrix + gram_block
        spectral_bound = jnp.sqrt(lax.optimization_barrier(jnp.sum(end_matrix * end_matrix, axis=(1, 2))))
        precond = invert_scaled(end_matrix, spectral_bound)
        readout = lax.map(solve_head, (jnp.transpose(query_block, (1, 0, 2)), jnp.transpose(scaled, (1, 0, 2)), jnp.transpose(value_block, (1, 0, 2)), base_matrix, precond, prior_cross))
        merged = jnp.transpose(readout, (1, 0, 2)).reshape(TOK_DEV, HEADS * DH)
        return ((prior_gram + gram_block, prior_cross + cross_block), merged)
    empty_state = jnp.zeros((HEADS, DH, DH), jnp.float32)
    final_carry, outputs = lax.scan(block_step, (empty_state, empty_state), (query_rows.reshape(split_shape), key_rows.reshape(split_shape), value_rows.reshape(split_shape)))
    return outputs.reshape(block_count * TOK_DEV, HEADS * DH)
```

```python
import functools

import jax
import jax.numpy as jnp
from jax import lax
from jax.experimental import pallas as pl
from jax.experimental.pallas import tpu as pltpu
from jax.sharding import Mesh
from jax.sharding import PartitionSpec as P

DH = 128
NS_STEPS = 8
REFINE = 2
SEQ = ("seq_0", "seq_1", "seq_2")
MESH = pl.DeviceIdType.MESH
F32, BF16 = jnp.float32, jnp.bfloat16


def dot(a, b):
    return jnp.dot(a, b, preferred_element_type=F32)


def dot_general(a, b, left, right):
    return lax.dot_general(a, b, (((left,), (right,)), ((), ())), preferred_element_type=F32)


def split(x):
    high = x.astype(BF16)
    low = (x - high.astype(F32)).astype(BF16)
    return high, low


def side(x):
    return jnp.concatenate(split(x), axis=1)


def square(x):
    row = side(x)
    return jnp.concatenate([row, row], axis=0)


def fold(p):
    return p[:, :DH] + p[:, DH:]


def iota(shape, dim):
    return lax.broadcasted_iota(jnp.int32, shape, dim)


def pack_gram(gram):
    half = DH // 2
    top, bottom = gram[:half], gram[half:]
    r, c = iota((half, DH), 0), iota((half, DH), 1)
    rolled = pltpu.roll(bottom, half, 1)
    packed = jnp.where((c < half) & (r < c), rolled, top)
    diagonal = jnp.sum(jnp.where(c == r + half, bottom, 0.0), axis=0, keepdims=True)
    return packed, diagonal


def unpack_gram(packed, diagonal):
    half = DH // 2
    r, c = iota((half, DH), 0), iota((half, DH), 1)
    flipped = jnp.concatenate([packed, packed], axis=0).T
    upper_flip, lower_flip = flipped[:half], flipped[half:]
    top = jnp.where((c < half) & (r < c), upper_flip, packed)
    a22 = pltpu.roll(jnp.where(r < c, packed, upper_flip), half, 1)
    bottom = jnp.where(c < half, lower_flip, jnp.where(c == r + half, diagonal, a22))
    return jnp.concatenate([top, bottom], axis=0)


def kernel(
    dims, gain, ridge, q_hbm, k_hbm, v_hbm, o_hbm,
    q, k, v, o, ks, shi, slo, own, state, bcat, ycat, ccat,
    gp, gin, gt, gf, gs, gr, xp, xin, xt, xf, xs, xr,
    load_sem, out_sem, pair_send, pair_recv, send_sem, recv_sem,
):
    nz, ny, heads, tokens = dims
    chips = nz * ny
    pieces = 8 * heads
    mine = pieces // 2
    per = mine // chips
    z, y, core = (lax.axis_index(a) for a in SEQ)
    chip = z * ny + y
    base_piece = core * mine

    def where_is(j):
        return {"seq_0": j // ny, "seq_1": j % ny}

    loads = []
    for n, (src, dst) in enumerate(((k_hbm, k), (v_hbm, v), (q_hbm, q))):
        copy = pltpu.make_async_copy(src, dst, load_sem.at[n])
        copy.start()
        loads.append(copy)

    barrier = pltpu.get_barrier_semaphore()
    pl.semaphore_signal(barrier, inc=1, device_id={"seq_2": 1 - core}, device_id_type=MESH)

    @pl.loop(1, chips)
    def _(d):
        pl.semaphore_signal(
            barrier, inc=1, device_id=where_is((chip + d) % chips), device_id_type=MESH
        )

    loads[0].wait()
    loads[1].wait()
    for h in range(heads):
        cols = slice(h * DH, (h + 1) * DH)
        scaled = (k[:, cols].astype(F32) * gain[h]).astype(BF16)
        ks[:, cols] = scaled
        both = dot_general(scaled, jnp.concatenate([scaled, v[:, cols]], axis=1), 0, 0)
        gram, cross = both[:, :DH], both[:, DH:]
        own[h] = gram
        packed, diagonal = pack_gram(gram)
        rows = slice(h * 8, (h + 1) * 8)
        gp[rows, 0:8, :] = packed.reshape(8, 8, DH)
        gp[rows, 8:9, :] = jnp.broadcast_to(diagonal.reshape(1, 1, DH), (8, 1, DH))
        xp[rows] = cross.reshape(8, 16, DH)
    pl.semaphore_wait(barrier, chips)

    def to_partner(src, dst, n):
        return pltpu.make_async_remote_copy(
            src_ref=src, dst_ref=dst, send_sem=pair_send.at[n], recv_sem=pair_recv.at[n],
            device_id={"seq_2": 1 - core}, device_id_type=MESH,
        )

    def to_chip(src, dst, group, there, slot):
        return pltpu.make_async_remote_copy(
            src_ref=src, dst_ref=dst, send_sem=send_sem.at[group, there],
            recv_sem=recv_sem.at[group, slot], device_id=where_is(there), device_id_type=MESH,
        )

    def slot(ref, j):
        return ref.at[pl.ds(j * per, per)]

    def half_slot(ref, j):
        return ref.at[pl.ds(base_piece + j * per, per)]

    def outward(part, came, total, found, group):
        total[...] = part[pl.ds(base_piece, mine)] + came[pl.ds(base_piece, mine)]
        found[pl.ds(chip * per, per)] = total[pl.ds(chip * per, per)]

        @pl.loop(1, chips)
        def _(d):
            there = (chip + d) % chips
            to_chip(slot(total, there), slot(found, chip), group, there, chip).start()

    def homeward(total, found, sums, result, group):
        def body(j, running):
            @pl.when(j != chip)
            def _():
                to_chip(slot(total, j), slot(found, j), group, j, j).wait_recv()

            sums[pl.ds(j * per, per)] = running

            @pl.when(j != chip)
            def _():
                to_chip(slot(sums, j), half_slot(result, chip), group + 1, j, chip).start()

            @pl.when(j == chip)
            def _():
                result[pl.ds(base_piece + chip * per, per)] = running

            return running + found[pl.ds(j * per, per)]

        lax.fori_loop(0, chips, body, jnp.zeros((per,) + found.shape[1:], F32))

    def gather(sums, result, group):
        @pl.loop(1, chips)
        def _(d):
            there = (chip + d) % chips
            to_chip(slot(sums, there), half_slot(result, there), group + 1, there, there).wait_recv()

    def drain(total, sums, found, result, group):
        @pl.loop(1, chips)
        def _(d):
            there = (chip + d) % chips
            to_chip(slot(total, there), slot(found, chip), group, there, chip).wait_send()
            to_chip(slot(sums, there), half_slot(result, chip), group + 1, there, chip).wait_send()

    def my_half(ref):
        return ref.at[pl.ds(base_piece, mine)]

    gram_pair = to_partner(gp, gin, 0)
    gram_pair.start()
    cross_pair = to_partner(xp, xin, 1)
    cross_pair.start()
    gram_pair.wait_recv()
    outward(gp, gin, gt, gf, 0)
    homeward(gt, gf, gs, gr, 0)
    cross_pair.wait_recv()
    outward(xp, xin, xt, xf, 2)
    gather(gs, gr, 0)
    gram_back = to_partner(my_half(gr), my_half(gr), 2)
    gram_back.start()
    gram_back.wait_recv()

    second = core == 1
    eye = jnp.where(iota((DH, DH), 0) == iota((DH, DH), 1), 1.0, 0.0)
    for h in range(heads):
        rows = slice(h * 8, (h + 1) * 8)
        whole = gr[rows] + jnp.where(second, gin[rows], 0.0)
        prior = unpack_gram(whole[:, 0:8, :].reshape(DH // 2, DH), whole[0, 8:9, :])
        base = prior + ridge[h] * eye
        bcat[h] = square(base)
        end = base + own[h]
        total = jnp.sum(jnp.sum(end * end, axis=1, keepdims=True), axis=0, keepdims=True)
        inverse = 1.0 / jnp.sqrt(total)
        state[h, :DH] = eye
        state[h, DH:] = end * inverse
        own[h] = jnp.broadcast_to(inverse, (DH, DH))

    @pl.loop(0, NS_STEPS)
    def _(step):
        for h in range(heads):
            x = state[h]
            left = side(x)
            row = left[DH:]
            product = dot(left, jnp.concatenate([row, row], axis=0))
            state[h] = 2.0 * x - fold(product)

    for h in range(heads):
        ycat[h] = square(state[h, :DH] * own[h])

    homeward(xt, xf, xs, xr, 2)
    loads[2].wait()

    block = 256
    causal = iota((block, block), 0) >= iota((block, block), 1)

    def scores_of(high, keys, count):
        s = dot_general(high, keys, 1, 1)
        if count == 1:
            return jnp.where(causal, s, 0.0).astype(BF16)
        past = s[:, : (count - 1) * block].astype(BF16)
        return jnp.concatenate(
            [past, jnp.where(causal, s[:, (count - 1) * block :], 0.0).astype(BF16)], axis=1
        )

    def columns(h):
        return pl.ds(pl.multiple_of(h * DH, DH), DH)

    @pl.loop(0, heads // 2)
    def _(pair):
        for which in range(2):
            h = pair * 2 + which
            cols = columns(h)
            for r in range(tokens // block):
                rows = slice(r * block, (r + 1) * block)
                query = q[rows, cols]
                keys = ks[0 : (r + 1) * block, cols]
                solution = fold(dot(query, ycat[h, :DH]))
                for repeat in range(REFINE):
                    high, low = split(solution)
                    in_block = dot(scores_of(high, keys, r + 1), keys)
                    through = fold(dot(jnp.concatenate([high, low], axis=1), bcat[h]))
                    residual = query.astype(F32) - through - in_block
                    solution = solution + fold(dot(side(residual), ycat[h]))
                high, low = split(solution)
                shi[rows, cols] = high
                slo[rows, cols] = low

    gather(xs, xr, 2)
    cross_back = to_partner(my_half(xr), my_half(xr), 3)
    cross_back.start()
    cross_back.wait_recv()
    for h in range(heads):
        rows = slice(h * 8, (h + 1) * 8)
        ccat[h] = square((xr[rows] + jnp.where(second, xin[rows], 0.0)).reshape(DH, DH))

    @pl.loop(0, heads // 2)
    def _(pair):
        for which in range(2):
            h = pair * 2 + which
            cols = columns(h)
            for r in range(tokens // block):
                rows = slice(r * block, (r + 1) * block)
                high, low = shi[rows, cols], slo[rows, cols]
                seen = slice(0, (r + 1) * block)
                scores = scores_of(high, ks[seen, cols], r + 1)
                total = fold(dot(jnp.concatenate([high, low], axis=1), ccat[h])) + dot(
                    scores, v[seen, cols]
                )
                o[rows, cols] = total.astype(BF16)
        both = pl.ds(pl.multiple_of(pair * 2 * DH, 2 * DH), 2 * DH)
        pltpu.make_async_copy(o.at[:, both], o_hbm.at[:, both], out_sem.at[pair]).start()

    @pl.loop(0, heads // 2)
    def _(pair):
        both = pl.ds(pl.multiple_of(pair * 2 * DH, 2 * DH), 2 * DH)
        pltpu.make_async_copy(o.at[:, both], o_hbm.at[:, both], out_sem.at[pair]).wait()

    drain(gt, gs, gf, gr, 0)
    drain(xt, xs, xf, xr, 2)
    for copy in (gram_pair, cross_pair, gram_back, cross_back):
        copy.wait_send()


def body(dims, query_rows, key_rows, value_rows, key_gain, regularizer):
    tokens, width = query_rows.shape
    heads = key_gain.shape[0]
    nz, ny = dims
    chips = nz * ny
    pieces = 8 * heads
    mine = pieces // 2
    rows = pltpu.VMEM((tokens, width), BF16)

    def exchange(depth):
        whole = pltpu.VMEM((pieces, depth, DH), F32)
        half = pltpu.VMEM((mine, depth, DH), F32)
        return [whole, whole, half, half, half, whole]

    cat = pltpu.VMEM((heads, 2 * DH, 2 * DH), BF16)
    return pl.pallas_call(
        functools.partial(kernel, (nz, ny, heads, tokens)),
        out_shape=jax.ShapeDtypeStruct((tokens, width), BF16),
        in_specs=[pl.BlockSpec(memory_space=pltpu.SMEM)] * 2
        + [pl.BlockSpec(memory_space=pl.ANY)] * 3,
        out_specs=pl.BlockSpec(memory_space=pl.ANY),
        scratch_shapes=[rows] * 7
        + [pltpu.VMEM((heads, DH, DH), F32), pltpu.VMEM((heads, 2 * DH, DH), F32), cat, cat, cat]
        + exchange(9)
        + exchange(16)
        + [
            pltpu.SemaphoreType.DMA((3,)),
            pltpu.SemaphoreType.DMA((heads // 2,)),
            pltpu.SemaphoreType.DMA((4,)),
            pltpu.SemaphoreType.DMA((4,)),
            pltpu.SemaphoreType.DMA((4, chips)),
            pltpu.SemaphoreType.DMA((4, chips)),
        ],
        compiler_params=pltpu.CompilerParams(collective_id=0, has_side_effects=True),
    )(key_gain, regularizer, query_rows, key_rows, value_rows)


def solution(mesh):
    nz, ny, cores = 8, 4, 2
    torus = Mesh(
        mesh.devices.reshape(nz, ny, cores, mesh.shape["head"]), SEQ + ("head",)
    )
    in_specs = (P(SEQ, "head"), P(SEQ, "head"), P(SEQ, "head"), P("head"), P("head"))
    return jax.shard_map(
        functools.partial(body, (nz, ny)), mesh=torus, in_specs=in_specs,
        out_specs=P(SEQ, "head"), check_vma=False,
    )
```

```python
import functools

import jax
import jax.numpy as jnp
from jax import lax
from jax.experimental import pallas as pl
from jax.experimental.pallas import tpu as pltpu
from jax.sharding import Mesh
from jax.sharding import PartitionSpec as P

DH = 128
NS_STEPS = 8
REFINE = 2
SEQ = ("seq_0", "seq_1", "seq_2")
MESH = pl.DeviceIdType.MESH
F32, BF16 = jnp.float32, jnp.bfloat16


def dot(a, b):
    return jnp.dot(a, b, preferred_element_type=F32)


def dot_general(a, b, left, right):
    return lax.dot_general(a, b, (((left,), (right,)), ((), ())), preferred_element_type=F32)


def split(x):
    high = x.astype(BF16)
    low = (x - high.astype(F32)).astype(BF16)
    return high, low


def side(x):
    return jnp.concatenate(split(x), axis=1)


def square(x):
    row = side(x)
    return jnp.concatenate([row, row], axis=0)


def fold(p):
    return p[:, :DH] + p[:, DH:]


def iota(shape, dim):
    return lax.broadcasted_iota(jnp.int32, shape, dim)


def pack_gram(gram):
    half = DH // 2
    top, bottom = gram[:half], gram[half:]
    r, c = iota((half, DH), 0), iota((half, DH), 1)
    rolled = pltpu.roll(bottom, half, 1)
    packed = jnp.where((c < half) & (r < c), rolled, top)
    diagonal = jnp.sum(jnp.where(c == r + half, bottom, 0.0), axis=0, keepdims=True)
    return packed, diagonal


def unpack_gram(packed, diagonal):
    half = DH // 2
    r, c = iota((half, DH), 0), iota((half, DH), 1)
    flipped = jnp.concatenate([packed, packed], axis=0).T
    upper_flip, lower_flip = flipped[:half], flipped[half:]
    top = jnp.where((c < half) & (r < c), upper_flip, packed)
    a22 = pltpu.roll(jnp.where(r < c, packed, upper_flip), half, 1)
    bottom = jnp.where(c < half, lower_flip, jnp.where(c == r + half, diagonal, a22))
    return jnp.concatenate([top, bottom], axis=0)


def kernel(
    dims, gain, ridge, q_hbm, k_hbm, v_hbm, o,
    q, k, v, ks, shi, slo, own, state, bcat, ycat, ccat,
    gp, gin, gt, gf, gs, gr, ga, gn, xp, xin, xt, xf, xs, xr, xa, xn,
    load_sem, pair_send, pair_recv, send_sem, recv_sem, span_send, span_recv, ready,
):
    nz, ny, planes, heads, tokens = dims
    groups = nz // planes
    chips = planes * ny
    pieces = 8 * heads
    mine = pieces // 2
    per = mine // chips
    z, y, core = (lax.axis_index(a) for a in SEQ)
    group = z // planes
    chip = (z % planes) * ny + y
    base_piece = core * mine

    def where_is(j):
        return {"seq_0": group * planes + j // ny, "seq_1": j % ny}

    loads = []
    for n, (src, dst) in enumerate(((k_hbm, k), (v_hbm, v), (q_hbm, q))):
        copy = pltpu.make_async_copy(src, dst, load_sem.at[n])
        copy.start()
        loads.append(copy)

    barrier = pltpu.get_barrier_semaphore()
    pl.semaphore_signal(barrier, inc=1, device_id={"seq_2": 1 - core}, device_id_type=MESH)

    @pl.loop(1, chips)
    def _(d):
        pl.semaphore_signal(
            barrier, inc=1, device_id=where_is((chip + d) % chips), device_id_type=MESH
        )

    for n in range(1, groups):

        @pl.when(group + n < groups)
        def _(n=n):
            pl.semaphore_signal(
                barrier, inc=1, device_id={"seq_0": z + n * planes}, device_id_type=MESH
            )

    loads[0].wait()
    loads[1].wait()
    for h in range(heads):
        cols = slice(h * DH, (h + 1) * DH)
        scaled = (k[:, cols].astype(F32) * gain[h]).astype(BF16)
        ks[:, cols] = scaled
        both = dot_general(scaled, jnp.concatenate([scaled, v[:, cols]], axis=1), 0, 0)
        gram, cross = both[:, :DH], both[:, DH:]
        own[h] = gram
        packed, diagonal = pack_gram(gram)
        rows = slice(h * 8, (h + 1) * 8)
        gp[rows, 0:8, :] = packed.reshape(8, 8, DH)
        gp[rows, 8:9, :] = jnp.broadcast_to(diagonal.reshape(1, 1, DH), (8, 1, DH))
        xp[rows] = cross.reshape(8, 16, DH)
    pl.semaphore_wait(barrier, chips + group)
    for n in range(1, groups):

        @pl.when(group >= n)
        def _(n=n):
            pl.semaphore_signal(
                ready.at[n - 1], inc=1, device_id={"seq_0": z - n * planes}, device_id_type=MESH
            )

    def to_partner(src, dst, n):
        return pltpu.make_async_remote_copy(
            src_ref=src, dst_ref=dst, send_sem=pair_send.at[n], recv_sem=pair_recv.at[n],
            device_id={"seq_2": 1 - core}, device_id_type=MESH,
        )

    def to_chip(src, dst, way, there):
        return pltpu.make_async_remote_copy(
            src_ref=src, dst_ref=dst, send_sem=send_sem.at[way], recv_sem=recv_sem.at[way],
            device_id=where_is(there), device_id_type=MESH,
        )

    def slot(ref, j):
        return ref.at[pl.ds(j * per, per)]

    def half_slot(ref, j):
        return ref.at[pl.ds(base_piece + j * per, per)]

    def others(ref):
        return ref.at[pl.ds(0, (chips - 1) * per)]

    def outward(part, came, total, found, way):
        total[...] = part[pl.ds(base_piece, mine)] + came[pl.ds(base_piece, mine)]
        found[pl.ds(chip * per, per)] = total[pl.ds(chip * per, per)]

        @pl.loop(1, chips)
        def _(d):
            there = (chip + d) % chips
            to_chip(slot(total, there), slot(found, chip), way, there).start()

    def span(every, came, way, n):
        return pltpu.make_async_remote_copy(
            src_ref=every.at[pl.ds(0, per)], dst_ref=came.at[pl.ds((n - 1) * per, per)],
            send_sem=span_send.at[way // 2, n - 1], recv_sem=span_recv.at[way // 2, n - 1],
            device_id={"seq_0": z + n * planes}, device_id_type=MESH,
        )

    def homeward(total, found, sums, result, every, came, way):
        to_chip(others(total), others(found), way, chip).wait_recv()
        everything = found[pl.ds(0, per)]
        for j in range(1, chips):
            everything = everything + found[pl.ds(j * per, per)]
        every[pl.ds(0, per)] = everything

        def pass_on():
            for n in range(1, groups):

                @pl.when(group + n < groups)
                def _(n=n):
                    if way == 0:
                        pl.semaphore_wait(ready.at[n - 1], 1)
                    span(every, came, way, n).start()

        pl.when(group > 0)(pass_on)
        every[pl.ds(per, per)] = jnp.zeros_like(everything)
        for n in range(1, groups):

            @pl.when(group >= n)
            def _(n=n):
                span(every, came, way, n).wait_recv()
                every[pl.ds(per, per)] += came[pl.ds((n - 1) * per, per)]

        def body(j, running):
            sums[pl.ds(j * per, per)] = running

            @pl.when(j != chip)
            def _():
                to_chip(slot(sums, j), half_slot(result, chip), way + 1, j).start()

            @pl.when(j == chip)
            def _():
                result[pl.ds(base_piece + chip * per, per)] = running

            return running + found[pl.ds(j * per, per)]

        lax.fori_loop(0, chips, body, every[pl.ds(per, per)])
        pl.when(group == 0)(pass_on)

    def gather(sums, result, way):
        to_chip(others(sums), others(result), way + 1, chip).wait_recv()

    def drain(total, sums, found, result, every, came, way):
        to_chip(others(total), others(found), way, chip).wait_send()
        to_chip(others(sums), others(result), way + 1, chip).wait_send()
        for n in range(1, groups):

            @pl.when(group + n < groups)
            def _(n=n):
                span(every, came, way, n).wait_send()

    def my_half(ref):
        return ref.at[pl.ds(base_piece, mine)]

    gram_pair = to_partner(gp, gin, 0)
    gram_pair.start()
    cross_pair = to_partner(xp, xin, 1)
    cross_pair.start()
    gram_pair.wait_recv()
    outward(gp, gin, gt, gf, 0)
    homeward(gt, gf, gs, gr, ga, gn, 0)
    cross_pair.wait_recv()
    outward(xp, xin, xt, xf, 2)
    gather(gs, gr, 0)
    gram_back = to_partner(my_half(gr), my_half(gr), 2)
    gram_back.start()
    gram_back.wait_recv()

    second = core == 1
    eye = jnp.where(iota((DH, DH), 0) == iota((DH, DH), 1), 1.0, 0.0)
    for h in range(heads):
        rows = slice(h * 8, (h + 1) * 8)
        whole = gr[rows] + jnp.where(second, gin[rows], 0.0)
        prior = unpack_gram(whole[:, 0:8, :].reshape(DH // 2, DH), whole[0, 8:9, :])
        base = prior + ridge[h] * eye
        bcat[h] = square(base)
        end = base + own[h]
        total = jnp.sum(jnp.sum(end * end, axis=1, keepdims=True), axis=0, keepdims=True)
        inverse = 1.0 / jnp.sqrt(total)
        half = end * (0.5 * inverse)
        left = side(half)
        rest = half - fold(dot(left, jnp.concatenate([left, left], axis=0)))
        state[h, :DH] = eye - half
        state[h, DH:] = rest + rest
        own[h] = jnp.broadcast_to(inverse * float(2**NS_STEPS), (DH, DH))

    @pl.loop(1, NS_STEPS - 1)
    def _(step):
        for h in range(heads):
            x = state[h]
            left = side(x)
            row = left[DH:]
            rest = x - fold(dot(left, jnp.concatenate([row, row], axis=0)))
            state[h, :DH] = rest[:DH]
            state[h, DH:] = rest[DH:] + rest[DH:]

    for h in range(heads):
        x = state[h, :DH]
        rest = x - fold(dot(side(x), square(state[h, DH:])))
        ycat[h] = square(rest * own[h])

    loads[2].wait()
    block = 256
    causal = iota((block, block), 0) >= iota((block, block), 1)

    def scores_of(high, keys):
        s = dot_general(high, keys, 1, 1)
        count = keys.shape[0] // block
        if count == 1:
            return jnp.where(causal, s, 0.0).astype(BF16)
        past = s[:, : (count - 1) * block].astype(BF16)
        return jnp.concatenate(
            [past, jnp.where(causal, s[:, (count - 1) * block :], 0.0).astype(BF16)], axis=1
        )

    def columns(h):
        return pl.ds(pl.multiple_of(h * DH, DH), DH)

    def chains_of(pair):
        chains = []
        for r in reversed(range(tokens // block)):
            for which in range(2):
                chains.append((pair * 2 + which, r))
        places = [(slice(r * block, (r + 1) * block), columns(h)) for h, r in chains]
        seen = [(slice(0, (r + 1) * block), columns(h)) for h, r in chains]
        return [h for h, _ in chains], places, seen

    @pl.loop(0, heads // 2)
    def _(pair):
        @pl.when(pair == 1)
        def _():
            homeward(xt, xf, xs, xr, xa, xn, 2)

        hs, places, seen = chains_of(pair)
        query = [q[at] for at in places]
        keys = [ks[at] for at in seen]
        solutions = [fold(dot(x, ycat[h, :DH])) for x, h in zip(query, hs)]
        for repeat in range(REFINE):
            parts = [split(x) for x in solutions]
            scores = [scores_of(x[0], key) for x, key in zip(parts, keys)]
            through = [fold(dot(jnp.concatenate(x, axis=1), bcat[h])) for x, h in zip(parts, hs)]
            in_block = [dot(x, key) for x, key in zip(scores, keys)]
            residual = [
                x.astype(F32) - t - b for x, t, b in zip(query, through, in_block)
            ]
            solutions = [
                x + fold(dot(side(r), ycat[h])) for x, r, h in zip(solutions, residual, hs)
            ]
        for x, at in zip(solutions, places):
            shi[at], slo[at] = split(x)

    gather(xs, xr, 2)
    cross_back = to_partner(my_half(xr), my_half(xr), 3)
    cross_back.start()
    cross_back.wait_recv()
    for h in range(heads):
        rows = slice(h * 8, (h + 1) * 8)
        ccat[h] = square((xr[rows] + jnp.where(second, xin[rows], 0.0)).reshape(DH, DH))

    @pl.loop(0, heads // 2)
    def _(pair):
        hs, places, seen = chains_of(pair)
        high = [shi[at] for at in places]
        scores = [scores_of(x, ks[at]) for x, at in zip(high, seen)]
        past = [
            fold(dot(jnp.concatenate([x, slo[at]], axis=1), ccat[h]))
            for x, at, h in zip(high, places, hs)
        ]
        present = [dot(x, v[at]) for x, at in zip(scores, seen)]
        for a, b, at in zip(past, present, places):
            o[at] = (a + b).astype(BF16)

    drain(gt, gs, gf, gr, ga, gn, 0)
    drain(xt, xs, xf, xr, xa, xn, 2)
    for copy in (gram_pair, cross_pair, gram_back, cross_back):
        copy.wait_send()


def body(dims, query_rows, key_rows, value_rows, key_gain, regularizer):
    tokens, width = query_rows.shape
    heads = key_gain.shape[0]
    nz, ny, planes = dims
    chips = planes * ny
    groups = nz // planes
    pieces = 8 * heads
    mine = pieces // 2
    per = mine // chips
    rows = pltpu.VMEM((tokens, width), BF16)

    def exchange(depth):
        whole = pltpu.VMEM((pieces, depth, DH), F32)
        half = pltpu.VMEM((mine, depth, DH), F32)
        sums = pltpu.VMEM((2 * per, depth, DH), F32)
        came = pltpu.VMEM(((groups - 1) * per, depth, DH), F32)
        return [whole, whole, half, half, half, whole, sums, came]

    cat = pltpu.VMEM((heads, 2 * DH, 2 * DH), BF16)
    return pl.pallas_call(
        functools.partial(kernel, (nz, ny, planes, heads, tokens)),
        out_shape=pltpu.VMEM((tokens, width), BF16),
        in_specs=[pl.BlockSpec(memory_space=pltpu.SMEM)] * 2
        + [pl.BlockSpec(memory_space=pl.ANY)] * 3,
        out_specs=pl.BlockSpec(memory_space=pltpu.VMEM),
        scratch_shapes=[rows] * 6
        + [pltpu.VMEM((heads, DH, DH), F32), pltpu.VMEM((heads, 2 * DH, DH), F32), cat, cat, cat]
        + exchange(9)
        + exchange(16)
        + [
            pltpu.SemaphoreType.DMA((3,)),
            pltpu.SemaphoreType.DMA((4,)),
            pltpu.SemaphoreType.DMA((4,)),
            pltpu.SemaphoreType.DMA((4,)),
            pltpu.SemaphoreType.DMA((4,)),
            pltpu.SemaphoreType.DMA((2, groups - 1)),
            pltpu.SemaphoreType.DMA((2, groups - 1)),
            pltpu.SemaphoreType.REGULAR((groups - 1,)),
        ],
        compiler_params=pltpu.CompilerParams(collective_id=0, has_side_effects=True),
    )(key_gain, regularizer, query_rows, key_rows, value_rows)


def solution(mesh):
    nz, ny, cores, planes = 8, 4, 2, 2
    torus = Mesh(
        mesh.devices.reshape(nz, ny, cores, mesh.shape["head"]), SEQ + ("head",)
    )
    in_specs = (P(SEQ, "head"), P(SEQ, "head"), P(SEQ, "head"), P("head"), P("head"))
    return jax.shard_map(
        functools.partial(body, (nz, ny, planes)), mesh=torus, in_specs=in_specs,
        out_specs=P(SEQ, "head"), check_vma=False,
    )
```

```python
import functools

import jax
import jax.numpy as jnp
from jax import lax
from jax.experimental import pallas as pl
from jax.experimental.pallas import tpu as pltpu
from jax.sharding import Mesh
from jax.sharding import PartitionSpec as P

DH = 128
NS_STEPS = 8
REFINE = 2
SEQ = ("seq_0", "seq_1", "seq_2")
MESH = pl.DeviceIdType.MESH
F32, BF16 = jnp.float32, jnp.bfloat16


def dot(a, b):
    return jnp.dot(a, b, preferred_element_type=F32)


def dot_general(a, b, left, right):
    return lax.dot_general(a, b, (((left,), (right,)), ((), ())), preferred_element_type=F32)


def split(x):
    high = x.astype(BF16)
    low = (x - high.astype(F32)).astype(BF16)
    return high, low


def side(x):
    return jnp.concatenate(split(x), axis=1)


def square(x):
    row = side(x)
    return jnp.concatenate([row, row], axis=0)


def fold(p):
    return p[:, :DH] + p[:, DH:]


def iota(shape, dim):
    return lax.broadcasted_iota(jnp.int32, shape, dim)


def pack_gram(gram):
    half = DH // 2
    top, bottom = gram[:half], gram[half:]
    r, c = iota((half, DH), 0), iota((half, DH), 1)
    rolled = pltpu.roll(bottom, half, 1)
    packed = jnp.where((c < half) & (r < c), rolled, top)
    diagonal = jnp.sum(jnp.where(c == r + half, bottom, 0.0), axis=0, keepdims=True)
    return packed, diagonal


def unpack_gram(packed, diagonal):
    half = DH // 2
    r, c = iota((half, DH), 0), iota((half, DH), 1)
    flipped = jnp.concatenate([packed, packed], axis=0).T
    upper_flip, lower_flip = flipped[:half], flipped[half:]
    top = jnp.where((c < half) & (r < c), upper_flip, packed)
    a22 = pltpu.roll(jnp.where(r < c, packed, upper_flip), half, 1)
    bottom = jnp.where(c < half, lower_flip, jnp.where(c == r + half, diagonal, a22))
    return jnp.concatenate([top, bottom], axis=0)


def kernel(
    dims, gain_hbm, ridge_hbm, q_hbm, k_hbm, v_hbm, o,
    gain, ridge, q, k, v, ks, shi, slo, own, state, bcat, ycat, ccat,
    gp, gin, gt, gf, gs, gr, ga, gn, xp, xin, xt, xf, xs, xr, xa, xn,
    load_sem, pair_send, pair_recv, send_sem, recv_sem, span_send, span_recv, ready,
):
    nz, ny, planes, heads, tokens = dims
    groups = nz // planes
    chips = planes * ny
    pieces = 8 * heads
    mine = pieces // 2
    per = mine // chips
    z, y, core = (lax.axis_index(a) for a in SEQ)
    group = z // planes
    chip = (z % planes) * ny + y
    base_piece = core * mine

    def where_is(j):
        return {"seq_0": group * planes + j // ny, "seq_1": j % ny}

    barrier = pltpu.get_barrier_semaphore()
    pl.semaphore_signal(barrier, inc=1, device_id={"seq_2": 1 - core}, device_id_type=MESH)

    @pl.loop(1, chips)
    def _(d):
        pl.semaphore_signal(
            barrier, inc=1, device_id=where_is((chip + d) % chips), device_id_type=MESH
        )

    for n in range(1, groups):

        @pl.when(group + n < groups)
        def _(n=n):
            pl.semaphore_signal(
                barrier, inc=1, device_id={"seq_0": z + n * planes}, device_id_type=MESH
            )

    loads = []
    for n, (src, dst) in enumerate(((gain_hbm, gain), (k_hbm, k), (v_hbm, v), (ridge_hbm, ridge), (q_hbm, q))):
        copy = pltpu.make_async_copy(src, dst, load_sem.at[n])
        copy.start()
        loads.append(copy)

    for n in range(3):
        loads[n].wait()
    for h in range(heads):
        cols = slice(h * DH, (h + 1) * DH)
        scaled = (k[:, cols].astype(F32) * gain[h]).astype(BF16)
        ks[:, cols] = scaled
        both = dot_general(scaled, jnp.concatenate([scaled, v[:, cols]], axis=1), 0, 0)
        gram, cross = both[:, :DH], both[:, DH:]
        own[h] = gram
        packed, diagonal = pack_gram(gram)
        rows = slice(h * 8, (h + 1) * 8)
        gp[rows, 0:8, :] = packed.reshape(8, 8, DH)
        gp[rows, 8:9, :] = jnp.broadcast_to(diagonal.reshape(1, 1, DH), (8, 1, DH))
        xp[rows] = cross.reshape(8, 16, DH)
    pl.semaphore_wait(barrier, chips + group)
    for n in range(1, groups):

        @pl.when(group >= n)
        def _(n=n):
            pl.semaphore_signal(
                ready.at[n - 1], inc=1, device_id={"seq_0": z - n * planes}, device_id_type=MESH
            )

    def to_partner(src, dst, n):
        return pltpu.make_async_remote_copy(
            src_ref=src, dst_ref=dst, send_sem=pair_send.at[n], recv_sem=pair_recv.at[n],
            device_id={"seq_2": 1 - core}, device_id_type=MESH,
        )

    def to_chip(src, dst, way, there):
        return pltpu.make_async_remote_copy(
            src_ref=src, dst_ref=dst, send_sem=send_sem.at[way], recv_sem=recv_sem.at[way],
            device_id=where_is(there), device_id_type=MESH,
        )

    def slot(ref, j):
        return ref.at[pl.ds(j * per, per)]

    def half_slot(ref, j):
        return ref.at[pl.ds(base_piece + j * per, per)]

    def others(ref):
        return ref.at[pl.ds(0, (chips - 1) * per)]

    def outward(part, came, total, found, way):
        total[...] = part[pl.ds(base_piece, mine)] + came[pl.ds(base_piece, mine)]
        found[pl.ds(chip * per, per)] = total[pl.ds(chip * per, per)]

        @pl.loop(1, chips)
        def _(d):
            there = (chip + d) % chips
            to_chip(slot(total, there), slot(found, chip), way, there).start()

    def span(every, came, way, n):
        return pltpu.make_async_remote_copy(
            src_ref=every.at[pl.ds(0, per)], dst_ref=came.at[pl.ds((n - 1) * per, per)],
            send_sem=span_send.at[way // 2, n - 1], recv_sem=span_recv.at[way // 2, n - 1],
            device_id={"seq_0": z + n * planes}, device_id_type=MESH,
        )

    def pass_on(every, came, way):
        for n in range(1, groups):

            @pl.when(group + n < groups)
            def _(n=n):
                if way == 0:
                    pl.semaphore_wait(ready.at[n - 1], 1)
                span(every, came, way, n).start()

    def collect(total, found, every, way):
        to_chip(others(total), others(found), way, chip).wait_recv()
        everything = found[pl.ds(0, per)]
        for j in range(1, chips):
            everything = everything + found[pl.ds(j * per, per)]
        every[pl.ds(0, per)] = everything

    def homeward(found, sums, result, every, came, way):
        every[pl.ds(per, per)] = jnp.zeros((per,) + found.shape[1:], F32)
        for n in range(1, groups):

            @pl.when(group >= n)
            def _(n=n):
                span(every, came, way, n).wait_recv()
                every[pl.ds(per, per)] += came[pl.ds((n - 1) * per, per)]

        def body(j, running):
            sums[pl.ds(j * per, per)] = running

            @pl.when(j != chip)
            def _():
                to_chip(slot(sums, j), half_slot(result, chip), way + 1, j).start()

            @pl.when(j == chip)
            def _():
                result[pl.ds(base_piece + chip * per, per)] = running

            return running + found[pl.ds(j * per, per)]

        lax.fori_loop(0, chips, body, every[pl.ds(per, per)])

    def gather(sums, result, way):
        to_chip(others(sums), others(result), way + 1, chip).wait_recv()

    def drain(total, sums, found, result, every, came, way):
        to_chip(others(total), others(found), way, chip).wait_send()
        to_chip(others(sums), others(result), way + 1, chip).wait_send()
        for n in range(1, groups):

            @pl.when(group + n < groups)
            def _(n=n):
                span(every, came, way, n).wait_send()

    def my_half(ref):
        return ref.at[pl.ds(base_piece, mine)]

    def other_half(ref):
        return ref.at[pl.ds(mine - base_piece, mine)]

    gram_pair = to_partner(other_half(gp), other_half(gin), 0)
    gram_pair.start()
    gram_rest = to_partner(my_half(gp), my_half(gin), 4)
    gram_rest.start()
    cross_pair = to_partner(xp, xin, 1)
    cross_pair.start()
    gram_pair.wait_recv()
    outward(gp, gin, gt, gf, 0)
    cross_pair.wait_recv()
    outward(xp, xin, xt, xf, 2)
    collect(gt, gf, ga, 0)

    @pl.when(group > 0)
    def _():
        pass_on(ga, gn, 0)

    homeward(gf, gs, gr, ga, gn, 0)

    @pl.when(group == 0)
    def _():
        pass_on(ga, gn, 0)

    collect(xt, xf, xa, 2)
    pass_on(xa, xn, 2)
    gather(gs, gr, 0)
    gram_back = to_partner(my_half(gr), my_half(gr), 2)
    gram_back.start()
    gram_rest.wait_recv()
    loads[3].wait()
    gram_back.wait_recv()

    second = core == 1
    eye = jnp.where(iota((DH, DH), 0) == iota((DH, DH), 1), 1.0, 0.0)
    inverses = []
    for h in range(heads):
        rows = slice(h * 8, (h + 1) * 8)
        whole = gr[rows] + jnp.where(second, gin[rows], 0.0)
        prior = unpack_gram(whole[:, 0:8, :].reshape(DH // 2, DH), whole[0, 8:9, :])
        base = prior + ridge[h] * eye
        bcat[h] = square(base)
        end = base + own[h]
        own[h] = end
        total = jnp.sum(jnp.sum(end * end, axis=0, keepdims=True), axis=1, keepdims=True)
        inverses.append(1.0 / jnp.sqrt(total))
    for h in range(heads):
        half = own[h] * (0.5 * inverses[h])
        left = side(half)
        rest = half - fold(dot(left, jnp.concatenate([left, left], axis=0)))
        state[h, :DH] = eye - half
        state[h, DH:] = rest + rest
    for h in range(heads):
        own[h] = jnp.broadcast_to(inverses[h] * float(2**NS_STEPS), (DH, DH))

    homeward(xf, xs, xr, xa, xn, 2)

    @pl.loop(1, NS_STEPS - 1)
    def _(step):
        for h in range(heads):
            x = state[h]
            left = side(x)
            row = left[DH:]
            rest = x - fold(dot(left, jnp.concatenate([row, row], axis=0)))
            state[h, :DH] = rest[:DH]
            state[h, DH:] = rest[DH:] + rest[DH:]

    for h in range(heads):
        x = state[h, :DH]
        rest = x - fold(dot(side(x), square(state[h, DH:])))
        ycat[h] = square(rest * own[h])

    loads[4].wait()
    block = 256
    causal = iota((block, block), 0) >= iota((block, block), 1)

    def scores_of(high, keys):
        s = dot_general(high, keys, 1, 1)
        count = keys.shape[0] // block
        if count == 1:
            return jnp.where(causal, s, 0.0).astype(BF16)
        past = s[:, : (count - 1) * block].astype(BF16)
        return jnp.concatenate(
            [past, jnp.where(causal, s[:, (count - 1) * block :], 0.0).astype(BF16)], axis=1
        )

    def columns(h):
        return pl.ds(pl.multiple_of(h * DH, DH), DH)

    def chains_of(pair):
        chains = []
        for r in reversed(range(tokens // block)):
            for which in range(2):
                chains.append((pair * 2 + which, r))
        places = [(slice(r * block, (r + 1) * block), columns(h)) for h, r in chains]
        seen = [(slice(0, (r + 1) * block), columns(h)) for h, r in chains]
        return [h for h, _ in chains], places, seen

    cross_back = to_partner(my_half(xr), my_half(xr), 3)

    @pl.loop(0, heads // 2)
    def _(pair):
        @pl.when(pair == heads // 2 - 2)
        def _():
            gather(xs, xr, 2)
            cross_back.start()

        hs, places, seen = chains_of(pair)
        query = [q[at] for at in places]
        keys = [ks[at] for at in seen]
        solutions = [fold(dot(x, ycat[h, :DH])) for x, h in zip(query, hs)]
        for repeat in range(REFINE):
            parts = [split(x) for x in solutions]
            scores = [scores_of(x[0], key) for x, key in zip(parts, keys)]
            through = [fold(dot(jnp.concatenate(x, axis=1), bcat[h])) for x, h in zip(parts, hs)]
            in_block = [dot(x, key) for x, key in zip(scores, keys)]
            residual = [
                x.astype(F32) - t - b for x, t, b in zip(query, through, in_block)
            ]
            solutions = [
                x + fold(dot(side(r), ycat[h])) for x, r, h in zip(solutions, residual, hs)
            ]
        for x, at in zip(solutions, places):
            shi[at], slo[at] = split(x)

    cross_back.wait_recv()
    for h in range(heads):
        rows = slice(h * 8, (h + 1) * 8)
        ccat[h] = square((xr[rows] + jnp.where(second, xin[rows], 0.0)).reshape(DH, DH))

    @pl.loop(0, heads // 2)
    def _(pair):
        hs, places, seen = chains_of(pair)
        high = [shi[at] for at in places]
        scores = [scores_of(x, ks[at]) for x, at in zip(high, seen)]
        past = [
            fold(dot(jnp.concatenate([x, slo[at]], axis=1), ccat[h]))
            for x, at, h in zip(high, places, hs)
        ]
        present = [dot(x, v[at]) for x, at in zip(scores, seen)]
        for a, b, at in zip(past, present, places):
            o[at] = (a + b).astype(BF16)

    drain(gt, gs, gf, gr, ga, gn, 0)
    drain(xt, xs, xf, xr, xa, xn, 2)
    for copy in (gram_pair, gram_rest, cross_pair, gram_back, cross_back):
        copy.wait_send()


def body(dims, query_rows, key_rows, value_rows, key_gain, regularizer):
    tokens, width = query_rows.shape
    heads = key_gain.shape[0]
    nz, ny, planes = dims
    chips = planes * ny
    groups = nz // planes
    pieces = 8 * heads
    mine = pieces // 2
    per = mine // chips
    rows = pltpu.VMEM((tokens, width), BF16)

    def exchange(depth):
        whole = pltpu.VMEM((pieces, depth, DH), F32)
        half = pltpu.VMEM((mine, depth, DH), F32)
        sums = pltpu.VMEM((2 * per, depth, DH), F32)
        came = pltpu.VMEM(((groups - 1) * per, depth, DH), F32)
        return [whole, whole, half, half, half, whole, sums, came]

    cat = pltpu.VMEM((heads, 2 * DH, 2 * DH), BF16)
    return pl.pallas_call(
        functools.partial(kernel, (nz, ny, planes, heads, tokens)),
        out_shape=pltpu.VMEM((tokens, width), BF16),
        in_specs=[pl.BlockSpec(memory_space=pl.ANY)] * 5,
        out_specs=pl.BlockSpec(memory_space=pltpu.VMEM),
        scratch_shapes=[pltpu.SMEM((heads,), F32)] * 2
        + [rows] * 6
        + [pltpu.VMEM((heads, DH, DH), F32), pltpu.VMEM((heads, 2 * DH, DH), F32), cat, cat, cat]
        + exchange(9)
        + exchange(16)
        + [
            pltpu.SemaphoreType.DMA((5,)),
            pltpu.SemaphoreType.DMA((5,)),
            pltpu.SemaphoreType.DMA((5,)),
            pltpu.SemaphoreType.DMA((4,)),
            pltpu.SemaphoreType.DMA((4,)),
            pltpu.SemaphoreType.DMA((2, groups - 1)),
            pltpu.SemaphoreType.DMA((2, groups - 1)),
            pltpu.SemaphoreType.REGULAR((groups - 1,)),
        ],
        compiler_params=pltpu.CompilerParams(collective_id=0, has_side_effects=True),
    )(key_gain, regularizer, query_rows, key_rows, value_rows)


def solution(mesh):
    nz, ny, cores, planes = 8, 4, 2, 2
    torus = Mesh(
        mesh.devices.reshape(nz, ny, cores, mesh.shape["head"]), SEQ + ("head",)
    )
    in_specs = (P(SEQ, "head"), P(SEQ, "head"), P(SEQ, "head"), P("head"), P("head"))
    return jax.shard_map(
        functools.partial(body, (nz, ny, planes)), mesh=torus, in_specs=in_specs,
        out_specs=P(SEQ, "head"), check_vma=False,
    )
```

```python
import functools

import jax
import jax.numpy as jnp
from jax import lax
from jax.experimental import pallas as pl
from jax.experimental.pallas import tpu as pltpu
from jax.sharding import Mesh
from jax.sharding import PartitionSpec as P

DH = 128
NS_STEPS = 8
REFINE = 2
SEQ = ("seq_0", "seq_1", "seq_2")
MESH = pl.DeviceIdType.MESH
F32, BF16 = jnp.float32, jnp.bfloat16


def dot(a, b):
    return jnp.dot(a, b, preferred_element_type=F32)


def dot_general(a, b, left, right):
    return lax.dot_general(a, b, (((left,), (right,)), ((), ())), preferred_element_type=F32)


def split(x):
    high = x.astype(BF16)
    low = (x - high.astype(F32)).astype(BF16)
    return high, low


def side(x):
    return jnp.concatenate(split(x), axis=1)


def square(x):
    row = side(x)
    return jnp.concatenate([row, row], axis=0)


def fold(p):
    return p[:, :DH] + p[:, DH:]


def iota(shape, dim):
    return lax.broadcasted_iota(jnp.int32, shape, dim)


def pack_gram(gram):
    half = DH // 2
    top, bottom = gram[:half], gram[half:]
    r, c = iota((half, DH), 0), iota((half, DH), 1)
    rolled = pltpu.roll(bottom, half, 1)
    packed = jnp.where((c < half) & (r < c), rolled, top)
    diagonal = jnp.sum(jnp.where(c == r + half, bottom, 0.0), axis=0, keepdims=True)
    return packed, diagonal


def unpack_gram(packed, diagonal):
    half = DH // 2
    r, c = iota((half, DH), 0), iota((half, DH), 1)
    flipped = jnp.concatenate([packed, packed], axis=0).T
    upper_flip, lower_flip = flipped[:half], flipped[half:]
    top = jnp.where((c < half) & (r < c), upper_flip, packed)
    a22 = jnp.where(c > r + half, pltpu.roll(packed, half, 1), upper_flip)
    bottom = jnp.where(c < half, lower_flip, jnp.where(c == r + half, diagonal, a22))
    return jnp.concatenate([top, bottom], axis=0)


def kernel(
    dims, gain_hbm, ridge_hbm, q_hbm, k_hbm, v_hbm, o,
    gain, ridge, q, k, v, ks, shi, slo, own, state, bcat, ycat, ccat,
    gp, gin, gt, gf, gs, gr, ga, gn, xp, xin, xt, xf, xs, xr, xa, xn,
    load_sem, pair_send, pair_recv, send_sem, recv_sem, span_send, span_recv, ready,
):
    nz, ny, planes, heads, tokens = dims
    groups = nz // planes
    chips = planes * ny
    pieces = 8 * heads
    mine = pieces // 2
    per = mine // chips
    z, y, core = (lax.axis_index(a) for a in SEQ)
    group = z // planes
    chip = (z % planes) * ny + y
    base_piece = core * mine

    def where_is(j):
        return {"seq_0": group * planes + j // ny, "seq_1": j % ny}

    steps = [(a, b) for a in range(planes) for b in range(ny) if a or b]
    steps.sort(key=lambda s: -(s[0] + min(s[1], ny - s[1])))
    others_at = [((z + a) % planes) * ny + (y + b) % ny for a, b in steps]

    barrier = pltpu.get_barrier_semaphore()
    pl.semaphore_signal(barrier, inc=1, device_id={"seq_2": 1 - core}, device_id_type=MESH)

    @pl.loop(1, chips)
    def _(d):
        pl.semaphore_signal(
            barrier, inc=1, device_id=where_is((chip + d) % chips), device_id_type=MESH
        )

    for n in range(1, groups):

        @pl.when(group + n < groups)
        def _(n=n):
            pl.semaphore_signal(
                barrier, inc=1, device_id={"seq_0": z + n * planes}, device_id_type=MESH
            )

    loads = []
    moves = [(gain_hbm, gain)]
    for first in (1 - core, core):
        cols = pl.ds(pl.multiple_of(first * (heads // 2 * DH), DH), heads // 2 * DH)
        moves += [(k_hbm.at[:, cols], k.at[:, cols]), (v_hbm.at[:, cols], v.at[:, cols])]
    moves += [(ridge_hbm, ridge), (q_hbm, q)]
    for n, (src, dst) in enumerate(moves):
        copy = pltpu.make_async_copy(src, dst, load_sem.at[n])
        copy.start()
        loads.append(copy)

    def columns(h):
        return pl.ds(pl.multiple_of(h * DH, DH), DH)

    def states(first):
        for n in range(heads // 2):
            h = first + n
            cols = columns(h)
            scaled = (k[:, cols].astype(F32) * gain[h]).astype(BF16)
            ks[:, cols] = scaled
            both = dot_general(scaled, jnp.concatenate([scaled, v[:, cols]], axis=1), 0, 0)
            gram, cross = both[:, :DH], both[:, DH:]
            own[h] = gram
            packed, diagonal = pack_gram(gram)
            rows = pl.ds(h * 8, 8)
            gp[rows, 0:8, :] = packed.reshape(8, 8, DH)
            gp[rows, 8:9, :] = jnp.broadcast_to(diagonal.reshape(1, 1, DH), (8, 1, DH))
            xp[rows] = cross.reshape(8, 16, DH)

    def to_partner(src, dst, n):
        return pltpu.make_async_remote_copy(
            src_ref=src, dst_ref=dst, send_sem=pair_send.at[n], recv_sem=pair_recv.at[n],
            device_id={"seq_2": 1 - core}, device_id_type=MESH,
        )

    def to_chip(src, dst, way, there):
        return pltpu.make_async_remote_copy(
            src_ref=src, dst_ref=dst, send_sem=send_sem.at[way], recv_sem=recv_sem.at[way],
            device_id=where_is(there), device_id_type=MESH,
        )

    def slot(ref, j):
        return ref.at[pl.ds(j * per, per)]

    def half_slot(ref, j):
        return ref.at[pl.ds(base_piece + j * per, per)]

    def others(ref):
        return ref.at[pl.ds(0, (chips - 1) * per)]

    def outward(part, came, total, found, way):
        total[...] = part[pl.ds(base_piece, mine)] + came[pl.ds(base_piece, mine)]
        found[pl.ds(chip * per, per)] = total[pl.ds(chip * per, per)]

        for there in others_at:
            to_chip(slot(total, there), slot(found, chip), way, there).start()

    def span(every, came, way, n):
        return pltpu.make_async_remote_copy(
            src_ref=every.at[pl.ds(0, per)], dst_ref=came.at[pl.ds((n - 1) * per, per)],
            send_sem=span_send.at[way // 2, n - 1], recv_sem=span_recv.at[way // 2, n - 1],
            device_id={"seq_0": z + n * planes}, device_id_type=MESH,
        )

    def pass_on(every, came, way):
        for n in range(1, groups):

            @pl.when(group + n < groups)
            def _(n=n):
                if way == 0:
                    pl.semaphore_wait(ready.at[n - 1], 1)
                span(every, came, way, n).start()

    def collect(total, found, every, way):
        to_chip(others(total), others(found), way, chip).wait_recv()
        everything = found[pl.ds(0, per)]
        for j in range(1, chips):
            everything = everything + found[pl.ds(j * per, per)]
        every[pl.ds(0, per)] = everything

    def homeward(found, sums, result, every, came, way):
        every[pl.ds(per, per)] = jnp.zeros((per,) + found.shape[1:], F32)
        for n in range(1, groups):

            @pl.when(group >= n)
            def _(n=n):
                span(every, came, way, n).wait_recv()
                every[pl.ds(per, per)] += came[pl.ds((n - 1) * per, per)]

        running = every[pl.ds(per, per)]
        for j in range(chips):
            sums[pl.ds(j * per, per)] = running
            running = running + found[pl.ds(j * per, per)]
        for there in others_at:
            to_chip(slot(sums, there), half_slot(result, chip), way + 1, there).start()
        result[pl.ds(base_piece + chip * per, per)] = sums[pl.ds(chip * per, per)]

    def gather(sums, result, way):
        to_chip(others(sums), others(result), way + 1, chip).wait_recv()

    def drain(total, sums, found, result, every, came, way):
        to_chip(others(total), others(found), way, chip).wait_send()
        to_chip(others(sums), others(result), way + 1, chip).wait_send()
        for n in range(1, groups):

            @pl.when(group + n < groups)
            def _(n=n):
                span(every, came, way, n).wait_send()

    def my_half(ref):
        return ref.at[pl.ds(base_piece, mine)]

    def other_half(ref):
        return ref.at[pl.ds(mine - base_piece, mine)]

    for n in range(3):
        loads[n].wait()
    states((1 - core) * (heads // 2))
    pl.semaphore_wait(barrier, chips + group)
    gram_pair = to_partner(other_half(gp), other_half(gin), 0)
    gram_pair.start()
    cross_pair = to_partner(other_half(xp), other_half(xin), 1)
    cross_pair.start()
    for n in range(1, groups):

        @pl.when(group >= n)
        def _(n=n):
            pl.semaphore_signal(
                ready.at[n - 1], inc=1, device_id={"seq_0": z - n * planes}, device_id_type=MESH
            )

    for n in range(3, 5):
        loads[n].wait()
    states(core * (heads // 2))
    gram_rest = to_partner(my_half(gp), my_half(gin), 4)
    gram_rest.start()
    cross_rest = to_partner(my_half(xp), my_half(xin), 5)
    cross_rest.start()
    gram_pair.wait_recv()
    outward(gp, gin, gt, gf, 0)
    cross_pair.wait_recv()
    outward(xp, xin, xt, xf, 2)
    collect(gt, gf, ga, 0)

    @pl.when(group > 0)
    def _():
        pass_on(ga, gn, 0)

    homeward(gf, gs, gr, ga, gn, 0)

    @pl.when(group == 0)
    def _():
        pass_on(ga, gn, 0)

    collect(xt, xf, xa, 2)
    pass_on(xa, xn, 2)
    gather(gs, gr, 0)
    gram_back = to_partner(my_half(gr), my_half(gr), 2)
    gram_back.start()
    gram_rest.wait_recv()
    loads[-2].wait()

    second = core == 1
    eye = jnp.where(iota((DH, DH), 0) == iota((DH, DH), 1), 1.0, 0.0)
    def matrices(first):
        for n in range(heads // 2):
            h = first + n
            rows = pl.ds(h * 8, 8)
            whole = gr[rows] + jnp.where(second, gin[rows], 0.0)
            prior = unpack_gram(whole[:, 0:8, :].reshape(DH // 2, DH), whole[0, 8:9, :])
            base = prior + ridge[h] * eye
            bcat[h] = square(base)
            end = base + own[h]
            total = jnp.sum(jnp.sum(end * end, axis=0, keepdims=True), axis=1, keepdims=True)
            inverse = 1.0 / jnp.sqrt(total)
            left = side(end)
            squared = fold(dot(left, jnp.concatenate([left, left], axis=0)))
            half = end * (0.5 * inverse)
            state[h, :DH] = eye - half
            state[h, DH:] = half + half - squared * (0.5 * inverse * inverse)
            own[h] = jnp.broadcast_to(inverse * float(2**NS_STEPS), (DH, DH))

    matrices(core * (heads // 2))
    gram_back.wait_recv()
    matrices((1 - core) * (heads // 2))

    homeward(xf, xs, xr, xa, xn, 2)

    for h in [*range(heads)] * (NS_STEPS - 2):
        x = state[h]
        left = side(x)
        row = left[DH:]
        rest = x - fold(dot(left, jnp.concatenate([row, row], axis=0)))
        state[h, :DH] = rest[:DH]
        state[h, DH:] = rest[DH:] + rest[DH:]

    for h in range(heads):
        x = state[h, :DH]
        rest = x - fold(dot(side(x), square(state[h, DH:])))
        ycat[h] = square(rest * own[h])

    loads[-1].wait()
    block = 256
    causal = iota((block, block), 0) >= iota((block, block), 1)

    def scores_of(high, keys):
        s = dot_general(high, keys, 1, 1)
        count = keys.shape[0] // block
        if count == 1:
            return jnp.where(causal, s, 0.0).astype(BF16)
        past = s[:, : (count - 1) * block].astype(BF16)
        return jnp.concatenate(
            [past, jnp.where(causal, s[:, (count - 1) * block :], 0.0).astype(BF16)], axis=1
        )

    def mixed(scores, rows, parts, matrix):
        left = jnp.concatenate([scores, *parts], axis=1)
        padded = jnp.concatenate([rows, jnp.zeros_like(rows)], axis=1)
        return fold(dot(left, jnp.concatenate([padded, matrix], axis=0)))

    def chains_of(pair):
        chains = []
        for r in reversed(range(tokens // block)):
            for which in range(4):
                chains.append((pair * 4 + which, r))
        places = [(slice(r * block, (r + 1) * block), columns(h)) for h, r in chains]
        seen = [(slice(0, (r + 1) * block), columns(h)) for h, r in chains]
        return [h for h, _ in chains], places, seen

    cross_back = to_partner(my_half(xr), my_half(xr), 3)

    @pl.loop(0, heads // 4)
    def _(pair):
        @pl.when(pair == 1)
        def _():
            gather(xs, xr, 2)
            cross_back.start()

        hs, places, seen = chains_of(pair)
        query = [q[at] for at in places]
        keys = [ks[at] for at in seen]
        solutions = [fold(dot(x, ycat[h, :DH])) for x, h in zip(query, hs)]
        for repeat in range(REFINE):
            parts = [split(x) for x in solutions]
            scores = [scores_of(x[0], key) for x, key in zip(parts, keys)]
            residual = [
                x.astype(F32) - mixed(c, key, part, bcat[h])
                for x, c, key, part, h in zip(query, scores, keys, parts, hs)
            ]
            solutions = [
                x + fold(dot(side(r), ycat[h])) for x, r, h in zip(solutions, residual, hs)
            ]
        for x, at in zip(solutions, places):
            shi[at], slo[at] = split(x)

    cross_rest.wait_recv()
    cross_back.wait_recv()
    for h in range(heads):
        rows = slice(h * 8, (h + 1) * 8)
        ccat[h] = square((xr[rows] + jnp.where(second, xin[rows], 0.0)).reshape(DH, DH))

    @pl.loop(0, heads // 4)
    def _(pair):
        hs, places, seen = chains_of(pair)
        high = [shi[at] for at in places]
        scores = [scores_of(x, ks[at]) for x, at in zip(high, seen)]
        for x, c, at, there, h in zip(high, scores, places, seen, hs):
            o[at] = mixed(c, v[there], (x, slo[at]), ccat[h]).astype(BF16)

    drain(gt, gs, gf, gr, ga, gn, 0)
    drain(xt, xs, xf, xr, xa, xn, 2)
    for copy in (gram_pair, gram_rest, cross_pair, cross_rest, gram_back, cross_back):
        copy.wait_send()


def body(dims, query_rows, key_rows, value_rows, key_gain, regularizer):
    tokens, width = query_rows.shape
    heads = key_gain.shape[0]
    nz, ny, planes = dims
    chips = planes * ny
    groups = nz // planes
    pieces = 8 * heads
    mine = pieces // 2
    per = mine // chips
    rows = pltpu.VMEM((tokens, width), BF16)

    def exchange(depth):
        whole = pltpu.VMEM((pieces, depth, DH), F32)
        half = pltpu.VMEM((mine, depth, DH), F32)
        sums = pltpu.VMEM((2 * per, depth, DH), F32)
        came = pltpu.VMEM(((groups - 1) * per, depth, DH), F32)
        return [whole, whole, half, half, half, whole, sums, came]

    cat = pltpu.VMEM((heads, 2 * DH, 2 * DH), BF16)
    return pl.pallas_call(
        functools.partial(kernel, (nz, ny, planes, heads, tokens)),
        out_shape=pltpu.VMEM((tokens, width), BF16),
        in_specs=[pl.BlockSpec(memory_space=pl.ANY)] * 5,
        out_specs=pl.BlockSpec(memory_space=pltpu.VMEM),
        scratch_shapes=[pltpu.SMEM((heads,), F32)] * 2
        + [rows] * 6
        + [pltpu.VMEM((heads, DH, DH), F32), pltpu.VMEM((heads, 2 * DH, DH), F32), cat, cat, cat]
        + exchange(9)
        + exchange(16)
        + [
            pltpu.SemaphoreType.DMA((7,)),
            pltpu.SemaphoreType.DMA((6,)),
            pltpu.SemaphoreType.DMA((6,)),
            pltpu.SemaphoreType.DMA((4,)),
            pltpu.SemaphoreType.DMA((4,)),
            pltpu.SemaphoreType.DMA((2, groups - 1)),
            pltpu.SemaphoreType.DMA((2, groups - 1)),
            pltpu.SemaphoreType.REGULAR((groups - 1,)),
        ],
        compiler_params=pltpu.CompilerParams(collective_id=0, has_side_effects=True),
    )(key_gain, regularizer, query_rows, key_rows, value_rows)


def solution(mesh):
    nz, ny, cores, planes = 8, 4, 2, 2
    torus = Mesh(
        mesh.devices.reshape(nz, ny, cores, mesh.shape["head"]), SEQ + ("head",)
    )
    in_specs = (P(SEQ, "head"), P(SEQ, "head"), P(SEQ, "head"), P("head"), P("head"))
    return jax.shard_map(
        functools.partial(body, (nz, ny, planes)), mesh=torus, in_specs=in_specs,
        out_specs=P(SEQ, "head"), check_vma=False,
    )
```

```python
import functools

import jax
import jax.numpy as jnp
from jax import lax
from jax.experimental import pallas as pl
from jax.experimental.pallas import tpu as pltpu
from jax.sharding import Mesh
from jax.sharding import PartitionSpec as P

DH = 128
NS_STEPS = 8
REFINE = 2
SEQ = ("seq_0", "seq_1", "seq_2")
MESH = pl.DeviceIdType.MESH
F32, BF16 = jnp.float32, jnp.bfloat16


def dot(a, b):
    return jnp.dot(a, b, preferred_element_type=F32)


def dot_general(a, b, left, right):
    return lax.dot_general(a, b, (((left,), (right,)), ((), ())), preferred_element_type=F32)


def split(x):
    high = x.astype(BF16)
    low = (x - high.astype(F32)).astype(BF16)
    return high, low


def side(x):
    return jnp.concatenate(split(x), axis=1)


def square(x):
    row = side(x)
    return jnp.concatenate([row, row], axis=0)


def fold(p):
    return p[:, :DH] + p[:, DH:]


def iota(shape, dim):
    return lax.broadcasted_iota(jnp.int32, shape, dim)


def pack_gram(gram):
    half = DH // 2
    top, bottom = gram[:half], gram[half:]
    r, c = iota((half, DH), 0), iota((half, DH), 1)
    rolled = pltpu.roll(bottom, half, 1)
    packed = jnp.where((c < half) & (r < c), rolled, top)
    diagonal = jnp.sum(jnp.where(c == r + half, bottom, 0.0), axis=0, keepdims=True)
    return packed, diagonal


def unpack_gram(packed, diagonal):
    half = DH // 2
    r, c = iota((half, DH), 0), iota((half, DH), 1)
    flipped = jnp.concatenate([packed, packed], axis=0).T
    upper_flip, lower_flip = flipped[:half], flipped[half:]
    top = jnp.where((c < half) & (r < c), upper_flip, packed)
    a22 = jnp.where(c > r + half, pltpu.roll(packed, half, 1), upper_flip)
    bottom = jnp.where(c < half, lower_flip, jnp.where(c == r + half, diagonal, a22))
    return jnp.concatenate([top, bottom], axis=0)


def kernel(
    dims, gain_hbm, ridge_hbm, q_hbm, k_hbm, v_hbm, o,
    gain, ridge, q, k, v, ks, shi, slo, own, state, bcat, ycat, ccat,
    gp, gin, gt, gf, gs, gr, ga, gn, xp, xin, xt, xf, xs, xr, xa, xn,
    load_sem, pair_send, pair_recv, send_sem, recv_sem, span_send, span_recv, ready,
):
    nz, ny, planes, heads, tokens = dims
    groups = nz // planes
    chips = planes * ny
    pieces = 2 * heads
    mine = pieces // 2
    per = mine // chips
    z, y, core = (lax.axis_index(a) for a in SEQ)
    group = z // planes
    chip = (z % planes) * ny + y
    base_piece = core * mine

    def where_is(j):
        return {"seq_0": group * planes + j // ny, "seq_1": j % ny}

    steps = [(a, b) for a in range(planes) for b in range(ny) if a or b]
    steps.sort(key=lambda s: -(s[0] + min(s[1], ny - s[1])))
    others_at = [((z + a) % planes) * ny + (y + b) % ny for a, b in steps]

    barrier = pltpu.get_barrier_semaphore()
    pl.semaphore_signal(barrier, inc=1, device_id={"seq_2": 1 - core}, device_id_type=MESH)

    for there in others_at:
        pl.semaphore_signal(
            barrier, inc=1, device_id=where_is(there), device_id_type=MESH
        )

    for n in range(1, groups):

        @pl.when(group + n < groups)
        def _(n=n):
            pl.semaphore_signal(
                barrier, inc=1, device_id={"seq_0": z + n * planes}, device_id_type=MESH
            )

    loads = []
    moves = [(gain_hbm, gain)]
    for first in (1 - core, core):
        cols = pl.ds(pl.multiple_of(first * (heads // 2 * DH), DH), heads // 2 * DH)
        moves += [(k_hbm.at[:, cols], k.at[:, cols]), (v_hbm.at[:, cols], v.at[:, cols])]
    moves += [(ridge_hbm, ridge), (q_hbm, q)]
    for n, (src, dst) in enumerate(moves):
        copy = pltpu.make_async_copy(src, dst, load_sem.at[n])
        copy.start()
        loads.append(copy)

    def columns(h):
        return pl.ds(pl.multiple_of(h * DH, DH), DH)

    def states(first):
        for n in range(heads // 2):
            h = first + n
            cols = columns(h)
            scaled = (k[:, cols].astype(F32) * gain[h]).astype(BF16)
            ks[:, cols] = scaled
            both = dot_general(scaled, jnp.concatenate([scaled, v[:, cols]], axis=1), 0, 0)
            gram, cross = both[:, :DH], both[:, DH:]
            own[h] = gram
            packed, diagonal = pack_gram(gram)
            rows = pl.ds(h * 2, 2)
            gp[rows, 0:32, :] = packed.reshape(2, 32, DH)
            gp[rows, 32:33, :] = jnp.broadcast_to(diagonal.reshape(1, 1, DH), (2, 1, DH))
            xp[rows] = cross.reshape(2, 64, DH)

    def to_partner(src, dst, n):
        return pltpu.make_async_remote_copy(
            src_ref=src, dst_ref=dst, send_sem=pair_send.at[n], recv_sem=pair_recv.at[n],
            device_id={"seq_2": 1 - core}, device_id_type=MESH,
        )

    def to_chip(src, dst, way, there):
        return pltpu.make_async_remote_copy(
            src_ref=src, dst_ref=dst, send_sem=send_sem.at[way], recv_sem=recv_sem.at[way],
            device_id=where_is(there), device_id_type=MESH,
        )

    def slot(ref, j):
        return ref.at[pl.ds(j * per, per)]

    def half_slot(ref, j):
        return ref.at[pl.ds(base_piece + j * per, per)]

    def others(ref):
        return ref.at[pl.ds(0, (chips - 1) * per)]

    def outward(part, came, total, found, way):
        total[...] = part[pl.ds(base_piece, mine)] + came[pl.ds(base_piece, mine)]
        found[pl.ds(chip * per, per)] = total[pl.ds(chip * per, per)]

        for there in others_at:
            to_chip(slot(total, there), slot(found, chip), way, there).start()

    def span(every, came, way, n):
        return pltpu.make_async_remote_copy(
            src_ref=every.at[pl.ds(0, per)], dst_ref=came.at[pl.ds((n - 1) * per, per)],
            send_sem=span_send.at[way // 2, n - 1], recv_sem=span_recv.at[way // 2, n - 1],
            device_id={"seq_0": z + n * planes}, device_id_type=MESH,
        )

    def pass_on(every, came, way, first=1, last=None):
        for n in range(first, groups if last is None else last):

            @pl.when(group + n < groups)
            def _(n=n):
                if way == 0:
                    pl.semaphore_wait(ready.at[n - 1], 1)
                span(every, came, way, n).start()

    def collect(total, found, every, way):
        to_chip(others(total), others(found), way, chip).wait_recv()
        everything = found[pl.ds(0, per)]
        for j in range(1, chips):
            everything = everything + found[pl.ds(j * per, per)]
        every[pl.ds(0, per)] = everything

    def homeward(found, sums, result, every, came, way):
        every[pl.ds(per, per)] = jnp.zeros((per,) + found.shape[1:], F32)
        for n in range(1, groups):

            @pl.when(group >= n)
            def _(n=n):
                span(every, came, way, n).wait_recv()
                every[pl.ds(per, per)] += came[pl.ds((n - 1) * per, per)]

        running = every[pl.ds(per, per)]
        for j in range(chips):
            sums[pl.ds(j * per, per)] = running
            running = running + found[pl.ds(j * per, per)]
        for there in others_at:
            to_chip(slot(sums, there), half_slot(result, chip), way + 1, there).start()
        result[pl.ds(base_piece + chip * per, per)] = sums[pl.ds(chip * per, per)]

    def gather(sums, result, way):
        to_chip(others(sums), others(result), way + 1, chip).wait_recv()

    def drain(total, sums, found, result, every, came, way):
        to_chip(others(total), others(found), way, chip).wait_send()
        to_chip(others(sums), others(result), way + 1, chip).wait_send()
        for n in range(1, groups):

            @pl.when(group + n < groups)
            def _(n=n):
                span(every, came, way, n).wait_send()

    def my_half(ref):
        return ref.at[pl.ds(base_piece, mine)]

    def other_half(ref):
        return ref.at[pl.ds(mine - base_piece, mine)]

    for n in range(3):
        loads[n].wait()
    states((1 - core) * (heads // 2))
    pl.semaphore_wait(barrier, chips + group)
    gram_pair = to_partner(other_half(gp), other_half(gin), 0)
    gram_pair.start()
    cross_pair = to_partner(other_half(xp), other_half(xin), 1)
    cross_pair.start()
    for n in range(1, groups):

        @pl.when(group >= n)
        def _(n=n):
            pl.semaphore_signal(
                ready.at[n - 1], inc=1, device_id={"seq_0": z - n * planes}, device_id_type=MESH
            )

    for n in range(3, 5):
        loads[n].wait()
    states(core * (heads // 2))
    gram_rest = to_partner(my_half(gp), my_half(gin), 4)
    gram_rest.start()
    cross_rest = to_partner(my_half(xp), my_half(xin), 5)
    cross_rest.start()
    gram_pair.wait_recv()
    outward(gp, gin, gt, gf, 0)
    cross_pair.wait_recv()
    outward(xp, xin, xt, xf, 2)
    collect(gt, gf, ga, 0)

    @pl.when(group > 0)
    def _():
        pass_on(ga, gn, 0)

    homeward(gf, gs, gr, ga, gn, 0)

    @pl.when(group == 0)
    def _():
        pass_on(ga, gn, 0)

    collect(xt, xf, xa, 2)
    pass_on(xa, xn, 2)
    gather(gs, gr, 0)
    gram_back = to_partner(my_half(gr), my_half(gr), 2)
    gram_back.start()
    gram_rest.wait_recv()
    loads[-2].wait()

    second = core == 1
    eye = jnp.where(iota((DH, DH), 0) == iota((DH, DH), 1), 1.0, 0.0)
    def matrices(first):
        for n in range(heads // 2):
            h = first + n
            rows = pl.ds(h * 2, 2)
            whole = gr[rows] + jnp.where(second, gin[rows], 0.0)
            prior = unpack_gram(whole[:, 0:32, :].reshape(DH // 2, DH), whole[0, 32:33, :])
            base = prior + ridge[h] * eye
            bcat[h] = square(base)
            end = base + own[h]
            total = jnp.sum(jnp.sum(end * end, axis=0, keepdims=True), axis=1, keepdims=True)
            inverse = 1.0 / jnp.sqrt(total)
            left = side(end)
            squared = fold(dot(left, jnp.concatenate([left, left], axis=0)))
            half = end * (0.5 * inverse)
            state[h, :DH] = eye - half
            state[h, DH:] = half + half - squared * (0.5 * inverse * inverse)
            own[h] = jnp.broadcast_to(inverse * float(2**NS_STEPS), (DH, DH))

    matrices(core * (heads // 2))
    gram_back.wait_recv()
    matrices((1 - core) * (heads // 2))

    homeward(xf, xs, xr, xa, xn, 2)

    for h in [*range(heads)] * (NS_STEPS - 2):
        x = state[h]
        left = side(x)
        row = left[DH:]
        rest = x - fold(dot(left, jnp.concatenate([row, row], axis=0)))
        state[h, :DH] = rest[:DH]
        state[h, DH:] = rest[DH:] + rest[DH:]

    for h in range(heads):
        x = state[h, :DH]
        rest = x - fold(dot(side(x), square(state[h, DH:])))
        ycat[h] = square(rest * own[h])

    loads[-1].wait()
    block = 256
    causal = iota((block, block), 0) >= iota((block, block), 1)

    def scores_of(high, keys):
        s = dot_general(high, keys, 1, 1)
        count = keys.shape[0] // block
        if count == 1:
            return jnp.where(causal, s, 0.0).astype(BF16)
        past = s[:, : (count - 1) * block].astype(BF16)
        return jnp.concatenate(
            [past, jnp.where(causal, s[:, (count - 1) * block :], 0.0).astype(BF16)], axis=1
        )

    def mixed(scores, rows, parts, matrix):
        left = jnp.concatenate([scores, *parts], axis=1)
        padded = jnp.concatenate([rows, jnp.zeros_like(rows)], axis=1)
        return fold(dot(left, jnp.concatenate([padded, matrix], axis=0)))

    def chains_of(pair):
        chains = []
        for r in reversed(range(tokens // block)):
            for which in range(4):
                chains.append((pair * 4 + which, r))
        places = [(slice(r * block, (r + 1) * block), columns(h)) for h, r in chains]
        seen = [(slice(0, (r + 1) * block), columns(h)) for h, r in chains]
        return [h for h, _ in chains], places, seen

    cross_back = to_partner(my_half(xr), my_half(xr), 3)

    @pl.loop(0, heads // 4)
    def _(pair):
        @pl.when(pair == 1)
        def _():
            gather(xs, xr, 2)
            cross_back.start()

        hs, places, seen = chains_of(pair)
        query = [q[at] for at in places]
        keys = [ks[at] for at in seen]
        solutions = [fold(dot(x, ycat[h, :DH])) for x, h in zip(query, hs)]
        for repeat in range(REFINE):
            parts = [split(x) for x in solutions]
            scores = [scores_of(x[0], key) for x, key in zip(parts, keys)]
            residual = [
                x.astype(F32) - mixed(c, key, part, bcat[h])
                for x, c, key, part, h in zip(query, scores, keys, parts, hs)
            ]
            solutions = [
                x + fold(dot(side(r), ycat[h])) for x, r, h in zip(solutions, residual, hs)
            ]
        for x, at in zip(solutions, places):
            shi[at], slo[at] = split(x)

    cross_rest.wait_recv()
    cross_back.wait_recv()
    for h in range(heads):
        rows = slice(h * 2, (h + 1) * 2)
        ccat[h] = square((xr[rows] + jnp.where(second, xin[rows], 0.0)).reshape(DH, DH))

    @pl.loop(0, heads // 4)
    def _(pair):
        hs, places, seen = chains_of(pair)
        high = [shi[at] for at in places]
        scores = [scores_of(x, ks[at]) for x, at in zip(high, seen)]
        for x, c, at, there, h in zip(high, scores, places, seen, hs):
            o[at] = mixed(c, v[there], (x, slo[at]), ccat[h]).astype(BF16)

    drain(gt, gs, gf, gr, ga, gn, 0)
    drain(xt, xs, xf, xr, xa, xn, 2)
    for copy in (gram_pair, gram_rest, cross_pair, cross_rest, gram_back, cross_back):
        copy.wait_send()


def body(dims, query_rows, key_rows, value_rows, key_gain, regularizer):
    tokens, width = query_rows.shape
    heads = key_gain.shape[0]
    nz, ny, planes = dims
    chips = planes * ny
    groups = nz // planes
    pieces = 2 * heads
    mine = pieces // 2
    per = mine // chips
    rows = pltpu.VMEM((tokens, width), BF16)

    def exchange(depth):
        whole = pltpu.VMEM((pieces, depth, DH), F32)
        half = pltpu.VMEM((mine, depth, DH), F32)
        sums = pltpu.VMEM((2 * per, depth, DH), F32)
        came = pltpu.VMEM(((groups - 1) * per, depth, DH), F32)
        return [whole, whole, half, half, half, whole, sums, came]

    cat = pltpu.VMEM((heads, 2 * DH, 2 * DH), BF16)
    return pl.pallas_call(
        functools.partial(kernel, (nz, ny, planes, heads, tokens)),
        out_shape=pltpu.VMEM((tokens, width), BF16),
        in_specs=[pl.BlockSpec(memory_space=pl.ANY)] * 5,
        out_specs=pl.BlockSpec(memory_space=pltpu.VMEM),
        scratch_shapes=[pltpu.SMEM((heads,), F32)] * 2
        + [rows] * 6
        + [pltpu.VMEM((heads, DH, DH), F32), pltpu.VMEM((heads, 2 * DH, DH), F32), cat, cat, cat]
        + exchange(33)
        + exchange(64)
        + [
            pltpu.SemaphoreType.DMA((7,)),
            pltpu.SemaphoreType.DMA((6,)),
            pltpu.SemaphoreType.DMA((6,)),
            pltpu.SemaphoreType.DMA((4,)),
            pltpu.SemaphoreType.DMA((4,)),
            pltpu.SemaphoreType.DMA((2, groups - 1)),
            pltpu.SemaphoreType.DMA((2, groups - 1)),
            pltpu.SemaphoreType.REGULAR((groups - 1,)),
        ],
        compiler_params=pltpu.CompilerParams(collective_id=0, has_side_effects=True),
    )(key_gain, regularizer, query_rows, key_rows, value_rows)


def solution(mesh):
    nz, ny, cores, planes = 8, 4, 2, 2
    torus = Mesh(
        mesh.devices.reshape(nz, ny, cores, mesh.shape["head"]), SEQ + ("head",)
    )
    in_specs = (P(SEQ, "head"), P(SEQ, "head"), P(SEQ, "head"), P("head"), P("head"))
    return jax.shard_map(
        functools.partial(body, (nz, ny, planes)), mesh=torus, in_specs=in_specs,
        out_specs=P(SEQ, "head"), check_vma=False,
    )
```
